32 devices in a mesh: head: 2 (over core), blk: 4 (over z), rep: 4 (over y, x).
Axes of the slice: x: 2, y: 2, z: 4, core: 2. Of those that a mesh axis runs over, the one named last changes fastest.
Arguments:
- queries: bfloat16 [2048, 768], P(('blk', 'rep'), 'head'), may hold values from -400 to 400
- keys: bfloat16 [2048, 256], P(('blk', 'rep'), 'head'), may hold values from -6 to 6
- values: bfloat16 [2048, 256], P(('blk', 'rep'), 'head'), may hold values from -18 to 18
- stretch_order: int32 [16], replicated, may hold values from 0 to 15, each once
- out_weight: bfloat16 [768, 3072], P('head'), may hold values from -0.21875 to 0.21875
Outputs:
- mixed_rows: bfloat16 [2048, 3072], P(('blk', 'rep'), 'head')
- log_sum_exp: float32 [6, 2048], P('head', ('blk', 'rep'))
The draws below stay inside these ranges and needn't reach their ends.
Inputs may be any that keep to these rules, and one draw needn't show every extreme that they name: `stretch_order`: each stretch number appears once.
All inputs are finite; a program needn't handle non-finite values.
Results may differ from the reference program's by a relative error of at most 0.02.
Values may be sent and summed in bfloat16 or wider, within the bound.
A program may use at most 128 MiB of HBM per device.

```python
import math
import jax
import jax.numpy as jnp
from jax import lax

D = 3072
GROUP = 3
DH = 128
KVH_DEV = 1
TOK_DEV = 128
KV_HEADS = 2
QHEADS = 6
NCHUNKS = 16
SEQ = 2048
N_HEAD = 2


def draw_keys(key, part):
    drawn_keys = jnp.clip(jax.random.normal(jax.random.fold_in(key, 3), (SEQ, KV_HEADS * DH), jnp.float32), -6.0, 6.0)
    return drawn_keys.astype(jnp.bfloat16)


def draw_queries(key, part):
    drawn_queries = jnp.clip(2.0 * jax.random.normal(jax.random.fold_in(key, 5), (SEQ, QHEADS * DH), jnp.float32), -12.0, 12.0)
    return drawn_queries.astype(jnp.bfloat16)


def block_scale(stream_key, extent, pieces, least, top_value):
    def one(axis_at, blocks):
        draws = jax.random.uniform(jax.random.fold_in(jax.random.fold_in(stream_key, 6), axis_at), (blocks,), jnp.float32, least / len(pieces), top_value / len(pieces))
        return jnp.repeat(jnp.exp(draws), extent[axis_at] // blocks).reshape((-1,) + (1,) * (len(extent) - axis_at - 1))

    factor_of = one(*pieces[0])
    for cut in pieces[1:]:
        factor_of = factor_of * one(*cut)
    return factor_of


def normal_values(stream_key, extent, scale, limit, cuts=(), kind=jnp.bfloat16):
    loudness = block_scale(stream_key, extent, cuts, -0.22, 0.18) if cuts else 1.0
    array = jax.random.normal(stream_key, extent, jnp.float32) * scale * loudness
    return jnp.minimum(jnp.maximum(array, -limit), limit).astype(kind)


def setup_inputs(seed: int = 0) -> dict:
    splits = jax.random.split(jax.random.key(seed), 6)
    queries = draw_queries(jax.random.fold_in(splits[5], 71), 0)
    keys = draw_keys(jax.random.fold_in(splits[5], 71), 0)
    values = normal_values(splits[2], (SEQ, KV_HEADS * DH), 3.0, 18.0, ((0, 16), (1, 2)))
    stretch_order = jax.random.permutation(splits[3], NCHUNKS).astype(jnp.int32)
    out_weight = normal_values(splits[4], (QHEADS * DH, D), (QHEADS * DH) ** -0.5, 0.21875, ((0, 2),))
    return dict(queries=queries, keys=keys, values=values, stretch_order=stretch_order, out_weight=out_weight)


def reference(queries, keys, values, stretch_order, out_weight):
    seq_len = queries.shape[0]
    row_ids = jnp.arange(seq_len, dtype=jnp.int32)
    positions = stretch_order[row_ids // TOK_DEV].astype(jnp.int32) * TOK_DEV + row_ids % TOK_DEV
    query_heads = queries.astype(jnp.float32).reshape(seq_len, QHEADS, DH).transpose(1, 0, 2)
    key_heads = keys.astype(jnp.float32).reshape(seq_len, KV_HEADS, DH).transpose(1, 0, 2)
    value_heads = values.astype(jnp.float32).reshape(seq_len, KV_HEADS, DH).transpose(1, 0, 2)
    block_len = math.gcd(seq_len, 1024)
    block_count = seq_len // block_len
    factor = DH ** (-0.5)

    def one_block(flat_index):
        head_index = flat_index // block_count
        block_index = flat_index % block_count
        group_index = head_index // GROUP
        query_head = lax.dynamic_index_in_dim(query_heads, head_index, 0, keepdims=False)
        query_block = lax.dynamic_slice_in_dim(query_head, block_index * block_len, block_len, 0)
        key_head = lax.dynamic_index_in_dim(key_heads, group_index, 0, keepdims=False)
        value_head = lax.dynamic_index_in_dim(value_heads, group_index, 0, keepdims=False)
        query_pos = lax.dynamic_slice_in_dim(positions, block_index * block_len, block_len, 0)
        scores = jnp.dot(query_block, key_head.T, precision=lax.Precision.HIGHEST) * factor
        allowed = positions[None, :] <= query_pos[:, None]
        masked = jnp.where(allowed, scores, -jnp.inf)
        row_top = jnp.max(masked, axis=1)
        expanded = jnp.where(allowed, jnp.exp(scores - row_top[:, None]), 0.0)
        totals = jnp.sum(expanded, axis=1)
        weights = lax.optimization_barrier(expanded.astype(jnp.bfloat16)).astype(jnp.float32)
        attended = jnp.dot(weights, value_head, precision=lax.Precision.HIGHEST) / totals[:, None]
        return (attended.astype(jnp.bfloat16), row_top + jnp.log(totals))
    outputs, sums = lax.map(one_block, jnp.arange(QHEADS * block_count, dtype=jnp.int32))
    attended = outputs.reshape(QHEADS, seq_len, DH).transpose(1, 0, 2).reshape(seq_len, QHEADS * DH)
    log_sum_exp = sums.reshape(QHEADS, seq_len)
    width = KVH_DEV * GROUP * DH
    mixed = jnp.zeros((seq_len, out_weight.shape[1]), jnp.float32)
    for rank in range(N_HEAD):
        partial_value = jnp.dot(attended[:, rank * width:(rank + 1) * width].astype(jnp.float32), out_weight[rank * width:(rank + 1) * width].astype(jnp.float32), precision=lax.Precision.HIGHEST)
        mixed = mixed + lax.optimization_barrier(partial_value.astype(jnp.bfloat16)).astype(jnp.float32)
    return (mixed.astype(jnp.bfloat16), log_sum_exp)
```

```python
import functools
import math

import jax
import jax.numpy as jnp
from jax import lax
from jax.experimental import pallas as pl
from jax.experimental.pallas import tpu as pltpu
from jax.sharding import PartitionSpec as P

DH = 128
NEG_FILL = -1e30
MESH = pl.DeviceIdType.MESH
UNROLL_LIMIT = 8
FAR_FIRST = False
SWAP = True
FAR_DIAG = False
FAR_X = ()
FAR_Y = ()
VMEM_LIMIT = 24 * 1024 * 1024
DIRECT_DIAG = 3

TREES = (
    (
        (
            (-1, 0, 0, 0, 0, 1, 4, 4, 4, 8, 8, 7, 0, 12, 12, 7),
            (4, 0, 6, 7, -1, 4, 4, 4, 4, 8, 8, 7, 8, 12, 12, 7),
            (8, 0, 0, 11, 0, 1, 2, 11, -1, 8, 8, 8, 8, 12, 12, 11),
            (12, 0, 0, 15, 12, 4, 4, 4, 12, 13, 8, 15, -1, 12, 12, 12),
        ),
        (
            (-1, 0, 0, 0, 0, 4, 4, 3, 0, 8, 8, 8, 0, 12, 12, 7),
            (4, 0, 6, 7, -1, 4, 4, 4, 4, 8, 8, 7, 8, 12, 12, 11),
            (8, 0, 0, 2, 0, 1, 10, 11, -1, 8, 8, 8, 8, 12, 12, 11),
            (12, 0, 0, 0, 8, 4, 14, 4, 12, 13, 8, 15, -1, 12, 12, 12),
        ),
    ),
    (
        (
            (0, 4, 12, 7, 8, 1, 3, 6, 14, 13, 9, 11, 0, 5, 2, 10),
            (1, 3, 5, 11, 0, 13, 12, 7, 6, 14, 10, 8, 9, 0, 4, 2),
            (13, 9, 5, 8, 4, 2, 7, 11, 0, 12, 6, 10, 3, 1, 14, 0),
            (7, 5, 12, 0, 6, 11, 1, 10, 9, 2, 14, 13, 0, 4, 8, 3),
        ),
        (
            (0, 2, 8, 9, 13, 11, 3, 1, 14, 12, 7, 10, 4, 5, 0, 6),
            (0, 2, 6, 11, 0, 13, 5, 8, 7, 14, 10, 12, 4, 9, 3, 1),
            (11, 2, 6, 14, 4, 3, 9, 13, 0, 12, 7, 5, 10, 1, 8, 0),
            (4, 6, 11, 5, 7, 10, 3, 9, 1, 12, 8, 14, 0, 0, 2, 13),
        ),
    ),
)
WAITS = (
    (9, 3, 2, 8, 17, 16, 25, 6, 7, 5, 4, 24, 11, 10, 19, 21, 18, 15, 14, 20, 13, 12, 31, 30, 27, 26, 29, 28, 22, 23),
    (0, 13, 1, 10, 11, 12, 15, 14, 24, 25, 6, 2, 3, 4, 17, 5, 16, 7, 29, 28, 23, 22, 30, 31, 26, 27, 21, 20, 19, 18),
    (25, 9, 21, 8, 19, 18, 20, 23, 1, 22, 24, 0, 11, 10, 15, 13, 12, 27, 26, 14, 29, 28, 3, 2, 30, 31, 5, 4, 7, 6),
    (16, 27, 17, 29, 26, 30, 28, 0, 31, 1, 9, 18, 19, 8, 20, 21, 2, 3, 4, 5, 23, 22, 11, 13, 10, 12, 14, 15, 6, 7),
)


def project(att, weight, tok):
    out = None
    for g in range(att.shape[1] // tok):
        term = lax.dot_general(
            att[:, g * tok:(g + 1) * tok], weight[g * DH:(g + 1) * DH, :],
            (((0,), (0,)), ((), ())), preferred_element_type=jnp.float32,
        )
        out = term if out is None else out + term
    return out


def finish_kernel(own_ref, att, w_buf, sums_ref, mixed_ref, lse_ref):
    lse_ref[...] = sums_ref[...]
    other = project(att[1], w_buf[1], own_ref.shape[0])
    mixed_ref[...] = (own_ref[...] + other).astype(mixed_ref.dtype)


def kernel(
    spans, q_ref, k_ref, v_ref, order_hbm, w_ref, own_ref, att, w_buf, lse_ref,
    order_ref, q_buf, kv, qt, acc, top, total,
    local_sem, f_send, z_send, z_recv, x_send, x_recv, y_send, y_recv, d_send, d_recv,
    w_send, w_recv, a_send, a_recv,
):
    tok, width = q_ref.shape
    group = width // DH
    rows = group * tok
    half = own_ref.shape[1]
    head = lax.axis_index("head")
    b = lax.axis_index("blk")
    r = lax.axis_index("rep")
    other = 1 - head
    rep_x = r + 1 - 2 * (r % 2)
    rep_y = (r + 2) % 4
    rep_d = 3 - r

    def peer(s):
        upper = b // (spans // 2)
        folded = b + upper * (spans - 1 - 2 * b)
        place = s - (folded + spans - s) // spans
        if SWAP and spans == 4 and s >= 2:
            place = place + (5 - 2 * s) * (1 - (folded + spans - 1) // spans)
        return place + upper * (spans - 1 - 2 * place)

    def for_each(count, step, start=0):
        if count - start <= UNROLL_LIMIT:
            for s in range(start, count):
                step(s)
        else:
            def run(s, carry):
                step(s)
                return carry
            lax.fori_loop(start, count, run, 0)

    loads = [
        pltpu.make_async_copy(k_ref, kv.at[0, b, 0], local_sem.at[0]),
        pltpu.make_async_copy(v_ref, kv.at[0, b, 1], local_sem.at[1]),
        pltpu.make_async_copy(q_ref, q_buf, local_sem.at[2]),
        pltpu.make_async_copy(order_hbm, order_ref, local_sem.at[4]),
    ]
    for load in loads:
        load.start()
    barrier = pltpu.get_barrier_semaphore()

    pl.semaphore_signal(barrier, inc=1, device_id={"rep": rep_x}, device_id_type=MESH)
    pl.semaphore_signal(barrier, inc=1, device_id={"rep": rep_y}, device_id_type=MESH)
    pl.semaphore_signal(barrier, inc=1, device_id={"head": other}, device_id_type=MESH)
    if DIRECT_DIAG <= spans:
        pl.semaphore_signal(barrier, inc=1, device_id={"rep": rep_d}, device_id_type=MESH)
    at_end = (b == 0) | (b == spans - 1)
    far = spans - 1 - b

    @pl.when(b > 0)
    def _():
        pl.semaphore_signal(barrier, inc=1, device_id={"blk": b - 1}, device_id_type=MESH)

    @pl.when(b < spans - 1)
    def _():
        pl.semaphore_signal(barrier, inc=1, device_id={"blk": b + 1}, device_id_type=MESH)

    far_reps = [r] + [rep_d] * FAR_DIAG + [rep_x] * bool(FAR_X) + [rep_y] * bool(FAR_Y)

    @pl.when(at_end)
    def _():
        for place in far_reps:
            pl.semaphore_signal(barrier, inc=1, device_id={"blk": far, "rep": place}, device_id_type=MESH)

    inner = 2 - (spans - b) // spans - (b + 1) // spans
    line = inner + (2 - inner) * len(far_reps)

    loads[0].wait()
    loads[1].wait()
    pl.semaphore_wait(barrier, line + 3 + (DIRECT_DIAG <= spans))

    def remote(src, dst, send, recv, axis, place):
        return pltpu.make_async_remote_copy(
            src_ref=src, dst_ref=dst, send_sem=send, recv_sem=recv,
            device_id={axis: place}, device_id_type=MESH,
        )

    def z_arrival(p, c):
        return remote(kv.at[0, p, c], kv.at[0, p, c], z_send.at[0, c], z_recv.at[p, c], "blk", p)

    def is_far(p):
        return (p - b == spans - 1) | (b - p == spans - 1)

    def far_copy(j, c):
        recv = [z_recv, x_recv, y_recv, d_recv][j]
        return pltpu.make_async_remote_copy(
            src_ref=kv.at[0, b, c], dst_ref=kv.at[j, b, c],
            send_sem=f_send.at[j, c], recv_sem=recv.at[b, c],
            device_id={"blk": far, "rep": [r, rep_x, rep_y, rep_d][j]}, device_id_type=MESH,
        )

    def all_far(act, js=(0, 1, 2, 3)):
        @pl.when(at_end)
        def _():
            for j in js:
                for c in [(0, 1), FAR_X, FAR_Y, (0, 1) if FAR_DIAG else ()][j]:
                    act(far_copy(j, c))

    def unless_far(p, c, skipped, act, copy):
        if c in skipped:
            @pl.when(jnp.logical_not(is_far(p)))
            def _():
                act(copy)
        else:
            act(copy)

    def x_copy(p, c):
        return remote(kv.at[0, p, c], kv.at[1, p, c], x_send.at[p, c], x_recv.at[p, c], "rep", rep_x)

    def y_copy(p, c):
        return remote(kv.at[0, p, c], kv.at[2, p, c], y_send.at[p, c], y_recv.at[p, c], "rep", rep_y)

    def d_copy(p, c):
        return remote(
            kv.at[1 + c, p, c], kv.at[3, p, c], d_send.at[p, c], d_recv.at[p, c],
            "rep", rep_x if c else rep_y,
        )

    def d_direct(p, c):
        return remote(kv.at[0, p, c], kv.at[3, p, c], d_send.at[p, c], d_recv.at[p, c], "rep", rep_d)

    def start(copy):
        copy.start()

    def each_plane(p, act, kinds=(0, 1)):
        for c in kinds:
            unless_far(p, c, FAR_X, act, x_copy(p, c))
            unless_far(p, c, FAR_Y, act, y_copy(p, c))

    def hop(p, c, down):
        return remote(kv.at[0, p, c], kv.at[0, p, c], z_send.at[p, c + 2 * down], z_recv.at[p, c], "blk", b + 1 - 2 * down)

    def pass_on(p, act, kinds=(0, 1)):
        @pl.when((p >= b) & (b > 0) & (p - b < spans - 2))
        def _():
            for c in kinds:
                act(hop(p, c, 1))

        @pl.when((p <= b) & (b < spans - 1) & (b - p < spans - 2))
        def _():
            for c in kinds:
                act(hop(p, c, 0))

    if FAR_FIRST:
        all_far(start, (0,))
    pass_on(b, start)
    each_plane(b, start)
    if not FAR_FIRST:
        all_far(start, (0,))
    all_far(start, (3, 1, 2))

    w_local = pltpu.make_async_copy(
        w_ref.at[:, pl.ds(pl.multiple_of(head * half, DH), half)], w_buf.at[0], local_sem.at[3]
    )
    w_remote = remote(
        w_ref.at[:, pl.ds(pl.multiple_of(other * half, DH), half)], w_buf.at[1],
        w_send, w_recv, "head", other,
    )
    w_local.start()
    w_remote.start()

    loads[2].wait()
    loads[3].wait()
    for g in range(group):
        qt[:, g * tok:(g + 1) * tok] = (
            q_buf[:, g * DH:(g + 1) * DH].astype(jnp.float32).T.astype(jnp.bfloat16)
        )
    key_at = lax.broadcasted_iota(jnp.int32, (tok, rows), 0)
    query_at = lax.broadcasted_iota(jnp.int32, (tok, rows), 1) % tok
    lead = key_at - query_at
    mine = order_ref[b * 4 + r]
    factor = DH ** (-0.5) * math.log2(math.e)

    def attend(j, p, first=False):
        rep = [r, rep_x, rep_y, rep_d][j]
        scores = jnp.dot(kv[j, p, 0], qt[...], preferred_element_type=jnp.float32) * factor
        gap = (mine - order_ref[p * 4 + rep]) * tok
        scores = jnp.where(lead <= gap, scores, NEG_FILL)
        best = jnp.max(scores, axis=0, keepdims=True)
        if not first:
            before = top[...]
            best = jnp.maximum(best, before)
        weights = jnp.exp2(scores - best)
        part = jnp.sum(weights, axis=0, keepdims=True)
        numer = lax.dot_general(
            kv[j, p, 1], weights.astype(jnp.bfloat16), (((0,), (0,)), ((), ())),
            preferred_element_type=jnp.float32,
        )
        if first:
            total[...] = part
            acc[...] = numer
        else:
            shrink = jnp.exp2(before - best)
            total[...] = total[...] * shrink + part
            acc[...] = acc[...] * shrink + numer
        top[...] = best

    def from_line(s):
        p = peer(s)
        for c in (0, 1):
            z_arrival(p, c).wait_recv()
            pass_on(p, start, (c,))
            each_plane(p, start, (c,))
        if spans <= UNROLL_LIMIT and s >= DIRECT_DIAG:
            for c in (0, 1):
                unless_far(p, c, (0, 1) if FAR_DIAG else (), start, d_direct(p, c))

    def to_diagonal(p, direct=False):
        skipped = (0, 1) if FAR_DIAG else ()
        x_copy(p, 0).wait_recv()
        if not direct:
            unless_far(p, 0, skipped, start, d_copy(p, 0))
        y_copy(p, 1).wait_recv()
        if not direct:
            unless_far(p, 1, skipped, start, d_copy(p, 1))
        x_copy(p, 1).wait_recv()
        y_copy(p, 0).wait_recv()

    def from_diagonal(p):
        d_copy(p, 0).wait_recv()
        d_copy(p, 1).wait_recv()

    attend(0, b, True)
    if spans <= UNROLL_LIMIT:
        places = [b] + [peer(s) for s in range(1, spans)]
        for s in range(1, spans + 2):
            if s < spans:
                from_line(s)
            if s <= spans:
                to_diagonal(places[s - 1], s - 1 >= DIRECT_DIAG)
            if s < spans:
                attend(0, places[s])
            if s <= spans:
                attend(1, places[s - 1])
                attend(2, places[s - 1])
            if s >= 2:
                from_diagonal(places[s - 2])
                attend(3, places[s - 2])
    else:
        for_each(spans, from_line, 1)
        for_each(spans, to_diagonal)
        for_each(spans, from_diagonal)

        def near(s):
            attend(0, peer(s))

        def others(p):
            for j in (1, 2, 3):
                attend(j, p)

        for_each(spans, near, 1)
        for_each(spans, others)

    att[0] = (acc[...] / total[...]).astype(jnp.bfloat16)
    swap = remote(att.at[0], att.at[1], a_send, a_recv, "head", other)
    swap.start()
    sums = (top[...] + jnp.log2(total[...])) * math.log(2.0)
    for g in range(group):
        lse_ref[g:g + 1, :] = sums[:, g * tok:(g + 1) * tok]

    w_local.wait()
    own_ref[...] = project(att[0], w_buf[0], tok)
    w_remote.wait_recv()
    swap.wait_recv()

    def sent(copy):
        copy.wait_send()

    def finish(p):
        pass_on(p, sent)
        each_plane(p, sent)
        for c in (0, 1):
            unless_far(p, c, (0, 1) if FAR_DIAG else (), sent, d_copy(p, c))

    for_each(spans, finish)
    all_far(sent)
    w_remote.wait_send()
    swap.wait_send()


def shared(rows):
    return all(row == rows[0] for row in rows)


def quad_kernel(
    plan, q_ref, k_ref, v_ref, order_hbm, w_ref, own_ref, att, w_buf, lse_ref,
    order_ref, q_buf, kv, qt, acc, top, total,
    kv_sem, q_sem, order_sem, send_sem, recv_sem, ready,
    w_sem, a_sem,
):
    tok, width = q_ref.shape
    group = width // DH
    rows = group * tok
    half = own_ref.shape[1]
    head = lax.axis_index("head")
    b = lax.axis_index("blk")
    r = lax.axis_index("rep")
    other = 1 - head
    in_last = b // 3
    in_third = b // 2 - in_last
    in_second = b % 2 - in_last
    step_x = 1 - 2 * (r % 2)
    step_y = 2 - 4 * (r // 2)
    depth = b + r % 2 + r // 2
    mine_key = depth * 16 + b * 4 + r

    def pick(values):
        first, second, third, last = values
        if shared(values):
            return first
        return first + in_second * (second - first) + in_third * (third - first) + in_last * (last - first)

    def rep_at(rel):
        return r + (rel % 2) * step_x + (rel // 2) * step_y

    def key_of(code):
        place, rep = code // 4, rep_at(code % 4)
        return (place + rep % 2 + rep // 2) * 16 + place * 4 + rep

    def device(code):
        return {"blk": code // 4, "rep": rep_at(code % 4)}

    def padded(lists):
        longest = max(len(row) for row in lists)
        return [
            ([len(row) > i for row in lists], [row[i] if len(row) > i else row[0] if row else 0 for row in lists])
            for i in range(longest)
        ]

    def each(lists, act):
        for valid, codes in padded(lists):
            code = pick(codes)
            if all(valid):
                act(code)
            else:
                pl.when(pick([int(ok) for ok in valid]) == 1)(functools.partial(act, code))

    own = b * 4
    loads = [
        pltpu.make_async_copy(k_ref, kv.at[2 * own], kv_sem),
        pltpu.make_async_copy(v_ref, kv.at[2 * own + 1], kv_sem),
        pltpu.make_async_copy(q_ref, q_buf, q_sem),
        pltpu.make_async_copy(order_hbm, order_ref, order_sem),
    ]
    for load in loads:
        load.start()
    barrier = pltpu.get_barrier_semaphore()

    def greet(code):
        @pl.when(key_of(code) > mine_key)
        def _():
            pl.semaphore_signal(barrier, inc=1, device_id=device(code), device_id_type=MESH)

    each(plan["partners"], greet)

    pl.semaphore_signal(barrier, inc=1, device_id={"head": other}, device_id_type=MESH)

    earlier = 1
    for valid, codes in padded(plan["partners"]):
        code = pick(codes)
        below = (mine_key + 4096 - key_of(code)) // 4096
        earlier = earlier + below * (1 if all(valid) else pick([int(ok) for ok in valid]))
    pl.semaphore_wait(barrier, earlier)

    def announce(code):
        @pl.when(key_of(code) < mine_key)
        def _():
            pl.semaphore_signal(
                ready.at[b * 4 + code % 4], inc=1, device_id=device(code), device_id_type=MESH
            )

    each(plan["sources"], announce)

    def send(slot, c, code, target, bucket):
        return pltpu.make_async_remote_copy(
            src_ref=kv.at[2 * slot + c], dst_ref=kv.at[2 * target + c],
            send_sem=send_sem.at[bucket], recv_sem=recv_sem.at[2 * target + c],
            device_id=device(code), device_id_type=MESH,
        )

    pltpu.make_async_copy(kv.at[pl.ds(2 * own, 2)], kv.at[pl.ds(2 * own, 2)], kv_sem).wait()

    def spread(code, c):
        send(own, c, code, own + code % 4, 0).start()

    def spread_lower(entry):
        code = entry // 2
        @pl.when(key_of(code) < mine_key)
        def _():
            spread(code, entry % 2)

    each(plan["own"], spread_lower)

    loads[2].wait()
    loads[3].wait()
    for g in range(group):
        qt[:, g * tok:(g + 1) * tok] = (
            q_buf[:, g * DH:(g + 1) * DH].astype(jnp.float32).T.astype(jnp.bfloat16)
        )
    key_at = lax.broadcasted_iota(jnp.int32, (tok, rows), 0)
    query_at = lax.broadcasted_iota(jnp.int32, (tok, rows), 1) % tok
    lead = key_at - query_at
    mine = order_ref[b * 4 + r]
    factor = DH ** (-0.5) * math.log2(math.e)

    def attend(slot, first=False):
        scores = jnp.dot(kv[2 * slot], qt[...], preferred_element_type=jnp.float32) * factor
        gap = (mine - order_ref[slot // 4 * 4 + rep_at(slot % 4)]) * tok
        scores = jnp.where(lead <= gap, scores, NEG_FILL)
        best = jnp.max(scores, axis=0, keepdims=True)
        if not first:
            before = top[...]
            best = jnp.maximum(best, before)
        weights = jnp.exp2(scores - best)
        part = jnp.sum(weights, axis=0, keepdims=True)
        numer = lax.dot_general(
            kv[2 * slot + 1], weights.astype(jnp.bfloat16), (((0,), (0,)), ((), ())),
            preferred_element_type=jnp.float32,
        )
        if first:
            total[...] = part
            acc[...] = numer
        else:
            shrink = jnp.exp2(before - best)
            total[...] = total[...] * shrink + part
            acc[...] = acc[...] * shrink + numer
        top[...] = best

    attend(own, True)

    def await_ready(code):
        @pl.when(key_of(code) > mine_key)
        def _():
            pl.semaphore_wait(ready.at[code], 1)

    def spread_upper(entry):
        code = entry // 4
        @pl.when(key_of(code) > mine_key)
        def _():
            @pl.when(entry // 2 % 2 == 1)
            def _():
                pl.semaphore_wait(ready.at[code], 1)
            spread(code, entry % 2)

    each(plan["own_upper"], spread_upper)
    each(plan["other_ready"], await_ready)

    def remote(src, dst, sems):
        return pltpu.make_async_remote_copy(
            src_ref=src, dst_ref=dst, send_sem=sems.at[0], recv_sem=sems.at[1],
            device_id={"head": other}, device_id_type=MESH,
        )

    w_local = pltpu.make_async_copy(
        w_ref.at[:, pl.ds(pl.multiple_of(head * half, DH), half)], w_buf.at[0], w_sem.at[2]
    )
    w_remote = remote(w_ref.at[:, pl.ds(pl.multiple_of(other * half, DH), half)], w_buf.at[1], w_sem)
    w_local.start()
    w_remote.start()

    done = 0
    for at, (slots, halves, children) in enumerate(plan["steps"]):
        slot, c = pick(slots), pick(halves)
        send(slot, c, 0 * b, slot, 0).wait_recv()

        def forward(entry):
            code = entry // 16
            send(slot, c, code, entry % 16, 1).start()

        each(children, forward)
        while done < len(plan["blocks"]) and plan["blocks"][done][0] <= at:
            attend(pick(plan["blocks"][done][1]))
            done += 1

    att[0] = (acc[...] / total[...]).astype(jnp.bfloat16)
    swap = remote(att.at[0], att.at[1], a_sem)
    swap.start()
    sums = (top[...] + jnp.log2(total[...])) * math.log(2.0)
    for g in range(group):
        lse_ref[g:g + 1, :] = sums[:, g * tok:(g + 1) * tok]

    w_local.wait()
    own_ref[...] = project(att[0], w_buf[0], tok)
    for place in range(4):
        @pl.when(b == place)
        def _():
            for bucket in (0, 1):
                count = plan["sent"][bucket][place]
                if count:
                    sent = kv.at[pl.ds(0, count)]
                    pltpu.make_async_copy(sent, sent, send_sem.at[bucket]).wait()
    w_remote.wait()
    swap.wait()


def make_plan():
    parents, ranks = TREES
    own, sources, sinks = [[] for _ in range(4)], [set() for _ in range(4)], [set() for _ in range(4)]
    forwards = {}
    for c in (0, 1):
        for z in range(4):
            for t in sorted((t for t in range(16) if t != z * 4), key=lambda t: ranks[c][z][t]):
                m = parents[c][z][t]
                place, rel = m // 4, m % 4
                code = t // 4 * 4 + (t % 4 ^ rel)
                sinks[place].add(code)
                sources[t // 4].add(place * 4 + (t % 4 ^ rel))
                if m == z * 4:
                    own[place].append((ranks[c][z][t], code, c))
                else:
                    forwards.setdefault((place, z * 4 + rel, c), []).append(code * 16 + z * 4 + t % 4)
    own = [[(code, c) for _, code, c in sorted(row)] for row in own]
    upper = []
    for p, row in enumerate(own):
        met, entries = set(), []
        for code, c in sorted(row, key=lambda e: abs(e[0] // 4 - p) + e[0] % 2 + e[0] // 2 % 2):
            entries.append(code * 4 + 2 * (code not in met) + c)
            met.add(code)
        upper.append(entries)
    steps, blocks = [], []
    for at in range(30):
        waits = [WAITS[p][at] for p in range(4)]
        steps.append((
            [w // 2 for w in waits], [w % 2 for w in waits],
            [forwards.get((p, waits[p] // 2, waits[p] % 2), []) for p in range(4)],
        ))
    complete = []
    for p in range(4):
        seen, row = set(), []
        for at, w in enumerate(WAITS[p]):
            if w // 2 in seen:
                row.append((at, w // 2))
            seen.add(w // 2)
        complete.append(row)
    for k in range(15):
        blocks.append((max(complete[p][k][0] for p in range(4)), [complete[p][k][1] for p in range(4)]))
    forwarded = [sum(len(v) for (place, _, _), v in forwards.items() if place == p) for p in range(4)]
    return {
        "partners": [sorted(sources[p] | sinks[p]) for p in range(4)],
        "sources": [sorted(sources[p]) for p in range(4)],
        "own": [[code * 2 + c for code, c in row] for row in own],
        "own_upper": upper,
        "other_ready": [sorted(sinks[p] - {code for code, _ in own[p]}) for p in range(4)],
        "steps": steps,
        "blocks": blocks,
        "sent": [[len(row) for row in own], forwarded],
    }


def solution(mesh):
    spans = mesh.shape["blk"]
    planned = spans == 4 and mesh.shape["rep"] == 4

    def body(queries, keys, values, stretch_order, out_weight):
        tok, width = queries.shape
        group = width // DH
        rows = group * tok
        half = out_weight.shape[1] // mesh.shape["head"]
        anywhere = pl.BlockSpec(memory_space=pltpu.HBM)
        vmem = pl.BlockSpec(memory_space=pltpu.VMEM)
        dma = pltpu.SemaphoreType.DMA
        regular = pltpu.SemaphoreType.REGULAR
        if planned:
            run = functools.partial(quad_kernel, make_plan())
            blocks = pltpu.VMEM((2 * 4 * spans, tok, DH), jnp.bfloat16)
            sems = [dma, dma, dma, dma((2,)), dma((32,)), regular((16,)), dma((3,)), dma((2,))]
        else:
            run = functools.partial(kernel, spans)
            blocks = pltpu.VMEM((4, spans, 2, tok, DH), jnp.bfloat16)
            sems = [
                dma((5,)), dma((4, 2)),
                dma((spans, 4)), dma((spans, 2)),
                dma((spans, 2)), dma((spans, 2)),
                dma((spans, 2)), dma((spans, 2)),
                dma((spans, 2)), dma((spans, 2)),
                dma, dma, dma, dma,
            ]
        gathered = pl.pallas_call(
            run,
            out_shape=(
                pltpu.VMEM((tok, half), jnp.float32),
                pltpu.VMEM((2, DH, rows), jnp.bfloat16),
                pltpu.VMEM((2, width, half), jnp.bfloat16),
                pltpu.VMEM((group, tok), jnp.float32),
            ),
            in_specs=[anywhere] * 5,
            out_specs=(vmem,) * 4,
            scratch_shapes=[
                pltpu.SMEM(stretch_order.shape, jnp.int32),
                pltpu.VMEM((tok, width), jnp.bfloat16),
                blocks,
                pltpu.VMEM((DH, rows), jnp.bfloat16),
                pltpu.VMEM((DH, rows), jnp.float32),
                pltpu.VMEM((1, rows), jnp.float32),
                pltpu.VMEM((1, rows), jnp.float32),
                *sems,
            ],
            compiler_params=pltpu.CompilerParams(collective_id=0, has_side_effects=True, vmem_limit_bytes=VMEM_LIMIT),
        )(*(
            pltpu.with_memory_space_constraint(array, pltpu.HBM)
            for array in (queries, keys, values, stretch_order, out_weight)
        ))
        return pl.pallas_call(
            finish_kernel,
            out_shape=(
                jax.ShapeDtypeStruct((tok, half), jnp.bfloat16),
                jax.ShapeDtypeStruct((group, tok), jnp.float32),
            ),
            in_specs=[vmem] * 4,
            out_specs=(vmem, vmem),
            compiler_params=pltpu.CompilerParams(vmem_limit_bytes=VMEM_LIMIT),
        )(*gathered)

    in_specs = (
        P(("blk", "rep"), "head"),
        P(("blk", "rep"), "head"),
        P(("blk", "rep"), "head"),
        P(),
        P("head", None),
    )
    out_specs = (P(("blk", "rep"), "head"), P("head", ("blk", "rep")))
    return jax.shard_map(body, mesh=mesh, in_specs=in_specs, out_specs=out_specs, check_vma=False)
```
